16 devices in a mesh: dp: 4 (over z, y), tp: 4 (over x, core).
Axes of the slice: x: 2, y: 2, z: 2, core: 2. Of those that a mesh axis runs over, the one named last changes fastest.
Arguments:
- enc_out: bfloat16 [32, 512, 4096], P('dp', 'tp'), parts along dimension 0
- norm_scale: bfloat16 [4096], replicated
- w_key: bfloat16 [4, 4096, 64, 64], P(None, None, 'tp')
- w_value: bfloat16 [4, 4096, 64, 64], P(None, None, 'tp')
Outputs:
- output 1: bfloat16 [4, 32, 512, 64, 64], P(None, 'dp', None, 'tp'), parts along dimension 1
- output 2: bfloat16 [4, 32, 512, 64, 64], P(None, 'dp', None, 'tp'), parts along dimension 1
There are 4 independent parts. The reference program is written for one: setup_inputs(seed, part) draws one part's arguments, and reference() takes and returns one part's arrays. A program takes and returns all parts, laid end to end along the dimension named above; an argument that names none is the same for every part.
All inputs are finite; a program needn't handle non-finite values.
Results may differ from the reference program's by a relative error of at most 0.001.
Values are sent between devices in bfloat16 or wider.
A program may use at most 1 GiB of HBM per device.

```python
import jax
import jax.numpy as jnp
from jax import lax

N_LAYERS = 4
BATCH_SIZE = 8
SEQ_LEN = 512
D_MODEL = 4096
N_HEADS = 64
HEAD_DIM = 64
NORM_EPS = 1e-6


def setup_inputs(seed: int = 0, part: int = 0) -> dict:
    root_key = jax.random.key(seed)
    k_act, k_norm, k_key, k_val = jax.random.split(root_key, 4)
    k_act = jax.random.fold_in(k_act, part)
    w_scale = D_MODEL ** -0.5
    w_shape = (N_LAYERS, D_MODEL, N_HEADS, HEAD_DIM)
    enc_out = jax.random.normal(k_act, (BATCH_SIZE, SEQ_LEN, D_MODEL), jnp.float32)
    norm_scale = jax.random.uniform(k_norm, (D_MODEL,), jnp.float32, 0.5, 1.5)
    w_key = jax.random.normal(k_key, w_shape, jnp.float32) * w_scale
    w_value = jax.random.normal(k_val, w_shape, jnp.float32) * w_scale
    return {"enc_out": enc_out.astype(jnp.bfloat16), "norm_scale": norm_scale.astype(jnp.bfloat16), "w_key": w_key.astype(jnp.bfloat16), "w_value": w_value.astype(jnp.bfloat16)}


def rms_norm(enc_out, norm_scale):
    acts = enc_out.astype(jnp.float32)
    mean_sq = jnp.mean(acts * acts, axis=-1, keepdims=True)
    return (acts * lax.rsqrt(mean_sq + NORM_EPS) * norm_scale.astype(jnp.float32)).astype(jnp.bfloat16)


def reference(enc_out, norm_scale, w_key, w_value):
    normed = rms_norm(enc_out, norm_scale).reshape(BATCH_SIZE * SEQ_LEN, D_MODEL)
    out_shape = (BATCH_SIZE, SEQ_LEN, N_HEADS, HEAD_DIM)

    def project(layer_weights):
        layer_key, layer_value = layer_weights
        keys = jnp.dot(normed, layer_key.reshape(D_MODEL, N_HEADS * HEAD_DIM), preferred_element_type=jnp.float32)
        values = jnp.dot(normed, layer_value.reshape(D_MODEL, N_HEADS * HEAD_DIM), preferred_element_type=jnp.float32)
        return keys.astype(jnp.bfloat16).reshape(out_shape), values.astype(jnp.bfloat16).reshape(out_shape)

    key_cache, value_cache = lax.map(project, (w_key, w_value))
    return key_cache, value_cache
```

```python
import functools

import jax
import jax.numpy as jnp
from jax import lax
from jax.experimental import pallas as pl
from jax.experimental.pallas import tpu as pltpu
from jax.sharding import PartitionSpec as P

NORM_EPS = 1e-6
LAYERS, D, ROWS = 4, 4096, 1024
TM = 512
STEPS = LAYERS * ROWS // TM
CH = 4
SEQ = 2
TOK = 128
BF16 = jnp.bfloat16
F32 = jnp.float32
VMEM = pltpu.VMEM
HBM = pltpu.HBM
DMA = pltpu.SemaphoreType.DMA

UNROLL = {"own_rest": 4, "near_a": 4, "near_b": 4, "far_a1": 4, "far_a2": 1, "far_b": 4}


def normed_rows(x, scale):
    acts = x.astype(F32)
    mean_sq = jnp.mean(acts * acts, axis=-1, keepdims=True)
    return (acts * lax.rsqrt(mean_sq + NORM_EPS) * scale).astype(BF16)


def w_copies(wk, wv, ring, wsem, step):
    return [pltpu.make_async_copy(w.at[step], ring.at[step % 2, i], wsem.at[i]) for i, w in enumerate((wk, wv))]


def out_copies(ok, ov, obuf, osem, step, slot, where, row0, chunks):
    copies = []
    row = pl.multiple_of((step % 2) * TM, TM)
    for c in chunks:
        lane = pl.multiple_of(where[row0 * CH + c] * TOK, TOK)
        first = where[(row0 + 1) * CH + c]
        for i, o in enumerate((ok, ov)):
            dst = o.at[step // 2, pl.ds(first, SEQ), pl.ds(row, TM), pl.ds(lane, TOK)]
            copies.append(pltpu.make_async_copy(obuf.at[slot, i, c], dst, osem.at[i * CH + c]))
    return copies


def project(ring, slot, y, obuf, c):
    tokens = y[c].reshape(SEQ * TOK, D)
    for i in range(2):
        out = lax.dot_general(ring[slot, i], tokens, (((1,), (1,)), ((), ())), preferred_element_type=F32).astype(BF16)
        for s in range(SEQ):
            obuf[slot, i, c, s] = out[:, s * TOK:(s + 1) * TOK]


def first_body(where, x_hbm, scale_ref, wk, wv, ok, ov, s0, s1, s2, s3, ring, obuf, y, xbuf, xsem, wsem, nsem, ssem):
    sends = (s0, s1, s2, s3)
    xcp = [pltpu.make_async_copy(x_hbm.at[pl.ds(c * SEQ, SEQ)], xbuf.at[c], xsem.at[c]) for c in range(CH)]
    scp = [pltpu.make_async_copy(y.at[c], sends[c], ssem.at[c]) for c in range(CH)]
    wcp = w_copies(wk, wv, ring, wsem, 0)
    ncp = w_copies(wk, wv, ring, nsem, 1)
    for cp in (xcp[0], wcp[0], xcp[1], wcp[1], xcp[2], xcp[3], *ncp):
        cp.start()
    scale = scale_ref[...].astype(F32)

    def norm_chunk(c):
        for s in range(SEQ):
            for r in range(0, TOK, 16):
                y[c, s, r:r + 16] = normed_rows(xbuf[c, s, r:r + 16], scale)

    xcp[0].wait()
    norm_chunk(0)
    wcp[0].wait()
    wcp[1].wait()
    for c in range(CH):
        scp[c].start()
        if c + 1 < CH:
            xcp[c + 1].wait()
            norm_chunk(c + 1)
        project(ring, 0, y, obuf, c)
    for cp in (*ncp, *scp):
        cp.wait()


def rest_body(s0, n, spot, prev, load, last, unroll, *refs):
    it = iter(refs)
    where = next(it)
    srcs = [next(it) for _ in range(CH)] if load else []
    wk, wv = next(it), next(it)
    for _ in range(5):
        next(it)
    ok, ov, ring, obuf, y, wsem, osem, ysem = it
    for c in range(len(srcs)):
        pltpu.make_async_copy(srcs[c], y.at[c], ysem.at[c]).start()

    def step(t, first):
        s = s0 + t
        slot = s % 2
        row0 = jnp.where(t == 0, 2 * prev, 2 * spot)
        leaving = out_copies(ok, ov, obuf, osem, (s + STEPS - 1) % STEPS, 1 - slot, where, row0, range(CH))
        for cp in leaving:
            cp.start()
        arriving = w_copies(wk, wv, ring, wsem, (s + 1) % STEPS)
        more = t + 1 < n if last else True

        def each(op):
            def run():
                for cp in arriving:
                    getattr(cp, op)()

            if last:
                pl.when(more)(run)
            else:
                run()

        each("start")
        if first:
            def chunk(c, _):
                pltpu.make_async_copy(srcs[0], y.at[c], ysem.at[c]).wait()
                project(ring, slot, y, obuf, c)
                return 0

            lax.fori_loop(0, CH, chunk, 0)
        elif unroll < CH:
            def group(g, _):
                for u in range(unroll):
                    project(ring, slot, y, obuf, g * unroll + u)
                return 0

            lax.fori_loop(0, CH // unroll, group, 0)
        else:
            for c in range(CH):
                project(ring, slot, y, obuf, c)
        for cp in leaving:
            cp.wait()
        each("wait")

    if load:
        step(jnp.int32(0), True)

    def body(t, _):
        step(t, False)
        return 0

    lax.fori_loop(1 if load else 0, n, body, 0)
    if last:
        end = out_copies(ok, ov, obuf, osem, s0 + n - 1, (s0 + n - 1) % 2, where, 2 * spot, range(CH))
        for cp in end:
            cp.start()
        for cp in end:
            cp.wait()


ANY_SPEC = pl.BlockSpec(memory_space=pl.ANY)
SMEM_SPEC = pl.BlockSpec(memory_space=pltpu.SMEM)
VMEM_SPEC = pl.BlockSpec(memory_space=VMEM)
CHUNK = (SEQ, TOK, D)
CACHE = (LAYERS, 4 * SEQ, ROWS, 4 * TOK)
RING = (2, 2, TM, D)
OBUF = (2, 2, CH, SEQ, TM, TOK)


def hbm(a):
    return pltpu.with_memory_space_constraint(a, HBM)


def cost(n):
    return pl.CostEstimate(flops=n * 2 * 2 * TM * D * CH * SEQ * TOK, bytes_accessed=n * 2 * TM * D * 2, transcendentals=0)


TOKENS = (CH,) + CHUNK


def first_call(where, x, scale, wk, wv):
    return pl.pallas_call(
        first_body,
        in_specs=[SMEM_SPEC, ANY_SPEC, VMEM_SPEC, ANY_SPEC, ANY_SPEC],
        out_specs=[ANY_SPEC] * (2 + CH) + [VMEM_SPEC] * 3,
        out_shape=[HBM(CACHE, BF16)] * 2 + [HBM(CHUNK, BF16)] * CH + [VMEM(RING, BF16), VMEM(OBUF, BF16), VMEM(TOKENS, BF16)],
        scratch_shapes=[VMEM(TOKENS, BF16), DMA((CH,)), DMA((2,)), DMA((2,)), DMA((CH,))],
        cost_estimate=cost(1), name="own_first",
        compiler_params=pltpu.CompilerParams(vmem_limit_bytes=35 * 2**20),
    )(where, hbm(x), scale, hbm(wk), hbm(wv))


def rest_call(s0, n, spot, prev, where, srcs, state, wk, wv, last=False, unroll=CH):
    held = [pltpu.with_memory_space_constraint(a, VMEM) for a in state[2:]]
    args = [where, *map(hbm, srcs), hbm(wk), hbm(wv), *map(hbm, state[:2]), *held]
    k = len(args) - len(state)
    return pl.pallas_call(
        functools.partial(rest_body, s0, n, spot, prev, bool(srcs), last, unroll),
        in_specs=[SMEM_SPEC] + [ANY_SPEC] * (k + 1) + [VMEM_SPEC] * 3,
        out_specs=[ANY_SPEC] * 2 + [VMEM_SPEC] * 3,
        out_shape=[HBM(CACHE, BF16)] * 2 + [VMEM(RING, BF16), VMEM(OBUF, BF16), VMEM(TOKENS, BF16)],
        input_output_aliases={k + i: i for i in range(len(state))},
        scratch_shapes=[DMA((2,)), DMA((2 * CH,)), DMA((CH,))],
        cost_estimate=cost(n),
        compiler_params=pltpu.CompilerParams(vmem_limit_bytes=35 * 2**20),
    )(*args)


def solution(mesh):
    def per_device(enc_out, norm_scale, w_key, w_value):
        wk, wv = (jnp.transpose(w, (0, 2, 3, 1)).reshape(STEPS, TM, D) for w in (w_key, w_value))
        me = lax.axis_index("tp").astype(jnp.int32)
        sib = [(i, i ^ 1) for i in range(4)]
        far = [(i, i ^ 2) for i in range(4)]
        flips = ((0, 0, 0, 0), (1, 1, 1, 1), (2, 2, 3, 3), (2, 2, 3, 3))
        firsts = ((0, 2, 4, 6), (0, 2, 4, 6), (0, 2, 0, 2), (4, 6, 4, 6))
        flip = jnp.array([f for a in flips for f in (*a, 0, 0, 0, 0)], jnp.int32)
        first = jnp.array([f for a in firsts for f in (0, 0, 0, 0, *a)], jnp.int32)
        here = jnp.array([1, 1, 1, 1, 0, 0, 0, 0] * 4, jnp.int32)
        where = (me ^ flip) * here + first

        r = first_call(where, enc_out, norm_scale.reshape(1, D), wk, wv)
        own, state = r[2:6], (*r[:2], *r[6:])
        direct, near, passed = [None] * 4, [None] * 4, [None] * 4
        for c in range(CH):
            direct[c] = lax.ppermute(own[c], "tp", far)
            near[c] = lax.ppermute(own[c], "tp", sib)
        for c in range(CH):
            passed[c] = lax.ppermute(direct[c], "tp", sib)
        ya = [direct[0], direct[1], passed[0], passed[1]]
        yb = [direct[2], direct[3], passed[2], passed[3]]
        plan = (
            ("own_rest", 1, 7, 0, 0, []),
            ("near_a", 0, 4, 1, 0, near),
            ("near_b", 4, 4, 1, 1, []),
            ("far_a1", 0, 6, 2, 1, ya),
            ("far_a2", 6, 2, 2, 2, []),
            ("far_b", 0, 8, 3, 2, yb),
        )
        for name, s0, n, spot, prev, srcs in plan:
            state = rest_call(s0, n, spot, prev, where, srcs, state, wk, wv, last=name == "far_b", unroll=UNROLL[name])
        return tuple(jnp.transpose(o.reshape(LAYERS, 8, 16, 64, 512), (0, 1, 4, 2, 3)) for o in state[:2])

    weight_spec = P(None, None, "tp", None)
    cache_spec = P(None, "dp", None, "tp", None)
    return jax.shard_map(per_device, mesh=mesh, in_specs=(P("dp", "tp", None), P(None), weight_spec, weight_spec), out_specs=(cache_spec, cache_spec), check_vma=False)
```
